32 devices in a mesh: rep: 4 (over z), fsdp: 8 (over y, x, core).
Axes of the slice: x: 2, y: 2, z: 4, core: 2. Of those that a mesh axis runs over, the one named last changes fastest.
Arguments:
- hidden: bfloat16 [8192, 7168], P(('rep', 'fsdp')), may hold values from -6 to 6
- out_grad: bfloat16 [8192, 2048], P(('rep', 'fsdp')), may hold values from -0.125 to 0.125
- inner_params: float32 [4, 7168, 2048], P('rep', 'fsdp'), may hold values from -0.132 to 0.132
- first_moment: bfloat16 [4, 7168, 2048], P('rep', 'fsdp'), may hold values from -6 to 6
- second_moment: bfloat16 [4, 7168, 2048], P('rep', 'fsdp'), may hold values from 0.049804688 to 2
- outer_params: float32 [7168, 2048], P('fsdp', 'rep'), may hold values from -0.12 to 0.12
- outer_momentum: float32 [7168, 2048], P('fsdp', 'rep'), may hold values from -0.012 to 0.012
Outputs:
- new_params: float32 [7168, 2048], P('fsdp')
- new_momentum: float32 [7168, 2048], P('fsdp', 'rep')
- new_first: bfloat16 [4, 7168, 2048], P('rep', 'fsdp')
- new_second: bfloat16 [4, 7168, 2048], P('rep', 'fsdp')
The draws below stay inside these ranges and needn't reach their ends.
All inputs are finite; a program needn't handle non-finite values.
Results may differ from the reference program's by a relative error of at most 0.009.
Values may be sent and summed in bfloat16 or wider, within the bound.
A program may use at most 192 MiB of HBM per device.

```python
import math
import jax
import jax.numpy as jnp
from jax import lax

FFW = 7168
DW = 2048
TOK_DEV = 256
INNER_STEP = 500
REPLICAS = 4
TOKENS = 8192
N_FSDP = 8


def base_weights(key):
    inner_key = jax.random.fold_in(key, 11)
    values = jax.random.normal(inner_key, (FFW, DW), jnp.float32)
    return jnp.clip(0.02 * values, -0.12, 0.12)


def draw_outer_params(key, part):
    return base_weights(key)


def draw_inner_params(key, part):
    drift_key = jax.random.fold_in(key, 13)
    drift = jax.random.normal(drift_key, (REPLICAS, FFW, DW), jnp.float32)
    drift = jnp.clip(0.002 * drift, -0.012, 0.012)
    return base_weights(key)[None] + drift


def with_spikes(array, stream_key, source, target, shards_of, factor):
    owner, partner = [(jnp.arange(array.shape[dim]) // (array.shape[dim] // shards_of)).reshape([-1 if axis == dim else 1 for axis in range(array.ndim)]) for dim in (source, target)]
    chosen = jax.random.permutation(stream_key, shards_of)[partner]
    strong = (owner == chosen) | (owner == (partner + shards_of // 2) % shards_of)
    return jnp.where(strong, factor * array, array)


def level_of(stream_key, extent, shards, smallest, top_value):
    def one(position, shards_of):
        draws = jax.random.uniform(jax.random.fold_in(jax.random.fold_in(stream_key, 6), position), (shards_of,), jnp.float32, smallest / len(shards), top_value / len(shards))
        return jnp.repeat(jnp.exp(draws), extent[position] // shards_of).reshape((-1,) + (1,) * (len(extent) - position - 1))

    level = one(*shards[0])
    for cut in shards[1:]:
        level = level * one(*cut)
    return level


def noise(own_key, shape, spread, most, cuts=(), kind=jnp.bfloat16):
    values = spread * jax.random.normal(own_key, shape, jnp.float32)
    if cuts:
        values = values * level_of(own_key, shape, cuts, -0.22, 0.18)
    return jnp.clip(values, -most, most).astype(kind)


def bell_draw_with(key, dims, deviation, most, pieces, heavy, held_as=jnp.bfloat16):
    result = deviation * jax.random.normal(key, dims, jnp.float32)
    if pieces:
        result = result * level_of(key, dims, pieces, -0.22, 0.18)
    return jnp.clip(with_spikes(result, jax.random.fold_in(key, 3), *heavy), -most, most).astype(held_as)


def setup_inputs(seed: int = 0) -> dict:
    streams_of = jax.random.split(jax.random.key(seed), 8)
    return {
        "hidden": bell_draw_with(streams_of[0], (TOKENS, FFW), 1.0, 6.0, ((0, 32),), (0, 1, 32, 2.75)),
        "out_grad": noise(streams_of[1], (TOKENS, DW), (TOK_DEV * N_FSDP) ** -0.5, 0.125, ((0, 32),)),
        "inner_params": draw_inner_params(jax.random.fold_in(streams_of[7], 71), 0),
        "first_moment": noise(streams_of[3], (REPLICAS, FFW, DW), 1.0, 6.0, ((0, 4), (1, 8))),
        "second_moment": jnp.clip(jnp.exp(math.log(2.0) - 3.6927934 * jax.random.uniform(streams_of[4], (REPLICAS, FFW, DW), jnp.float32) ** level_of(streams_of[4], (REPLICAS, FFW, DW), ((0, 4), (1, 8)), -0.2, 0.2)), 0.049804688, 2.0).astype(jnp.bfloat16),
        "outer_params": draw_outer_params(jax.random.fold_in(streams_of[7], 71), 0),
        "outer_momentum": noise(streams_of[6], (FFW, DW), 0.002, 0.012, ((0, 8), (1, 4)), jnp.float32),
    }


beta_one = 0.9
beta_two = 0.95
epsilon = 1e-08
inner_rate = 0.0004
weight_decay = 0.1
outer_rate = 0.7
nesterov = 0.9

def add_block(running, block_pair):
    hidden_block, grad_block = block_pair
    partial_value = jnp.dot(hidden_block.T, grad_block, preferred_element_type=jnp.float32)
    rounded = lax.optimization_barrier(partial_value.astype(jnp.bfloat16)).astype(jnp.float32)
    return (running + rounded, None)

def replica_step(running, inputs):
    hidden_blocks, grad_blocks, params, first_state, second = inputs
    gradient, unused = lax.scan(add_block, jnp.zeros((FFW, DW), jnp.float32), (hidden_blocks, grad_blocks))
    moment_one = beta_one * first_state.astype(jnp.float32) + (1.0 - beta_one) * gradient
    moment_two = beta_two * second.astype(jnp.float32) + (1.0 - beta_two) * gradient * gradient
    corrected_one = moment_one / (1.0 - beta_one ** INNER_STEP)
    corrected_two = moment_two / (1.0 - beta_two ** INNER_STEP)
    stepped = params - inner_rate * (corrected_one / (jnp.sqrt(corrected_two) + epsilon) + weight_decay * params)
    return (running + stepped, (moment_one.astype(jnp.bfloat16), moment_two.astype(jnp.bfloat16)))

def reference(hidden, out_grad, inner_params, first_moment, second_moment, outer_params, outer_momentum):
    hidden_blocks = hidden.reshape(REPLICAS, N_FSDP, TOK_DEV, FFW)
    grad_blocks = out_grad.reshape(REPLICAS, N_FSDP, TOK_DEV, DW)
    summed, moments = lax.scan(replica_step, jnp.zeros((FFW, DW), jnp.float32), (hidden_blocks, grad_blocks, inner_params, first_moment, second_moment))
    outer_delta = outer_params - summed / REPLICAS
    new_momentum = nesterov * outer_momentum + outer_delta
    new_params = outer_params - outer_rate * (outer_delta + nesterov * new_momentum)
    return (new_params, new_momentum, moments[0], moments[1])
```

```python
import functools

import jax
import jax.numpy as jnp
from jax import lax
from jax.experimental import pallas as pl
from jax.experimental.pallas import tpu as pltpu
from jax.sharding import PartitionSpec as P

INNER_STEP = 500

beta_one = 0.9
beta_two = 0.95
epsilon = 1e-08
inner_rate = 0.0004
weight_decay = 0.1
outer_rate = 0.7
nesterov = 0.9

WIRE = jnp.bfloat16
WIRE_SCALE = 16.0


def encode(value):
    scaled = value * WIRE_SCALE
    square = scaled * scaled
    fourth = square * square
    eighth = fourth * fourth
    return jnp.where(scaled < 0.0, -eighth, eighth).astype(WIRE)


def decode(coded):
    wide = coded.astype(jnp.float32)
    root = jnp.sqrt(jnp.sqrt(jnp.sqrt(jnp.abs(wide)))) * (1.0 / WIRE_SCALE)
    return jnp.where(wide < 0.0, -root, root)


def outer_kernel(
    n, chunks, step_ref, outer_ref, mom_ref, out_ref, newmom_ref,
    from_left, from_right, acc, total,
    rs_send, rs_left, rs_right, ag_right, ag_left, ag_recv,
):
    z = lax.axis_index("rep")
    rows, block = outer_ref.shape
    rc = rows // chunks
    has_left, has_right = z > 0, z < n - 1

    barrier = pltpu.get_barrier_semaphore()

    @pl.when(has_left)
    def _():
        pl.semaphore_signal(barrier, inc=1, device_id={"rep": z - 1})

    @pl.when(has_right)
    def _():
        pl.semaphore_signal(barrier, inc=1, device_id={"rep": z + 1})

    pl.semaphore_wait(barrier, has_left.astype(jnp.int32) + has_right.astype(jnp.int32))

    def part(c, o):
        start = o * block
        if not isinstance(o, int):
            start = pl.multiple_of(start, 128)
        return pl.ds(pl.multiple_of(c * rc, rc), rc), pl.ds(start, block)

    def send_sum(src, c, o, to_right):
        at = part(c, o)
        return pltpu.make_async_remote_copy(
            src_ref=src.at[at],
            dst_ref=(from_left if to_right else from_right).at[at],
            send_sem=rs_send.at[c, o],
            recv_sem=(rs_left if to_right else rs_right).at[c, o],
            device_id={"rep": z + 1 if to_right else z - 1},
        )

    def send_new(c, o, to_right):
        at = part(c, o)
        return pltpu.make_async_remote_copy(
            src_ref=out_ref.at[at],
            dst_ref=out_ref.at[at],
            send_sem=(ag_right if to_right else ag_left).at[c, o],
            recv_sem=ag_recv.at[c, o],
            device_id={"rep": z + 1 if to_right else z - 1},
        )

    def wave(c, to_right):
        first = z == 0 if to_right else z == n - 1
        order = range(n - 1, 0, -1) if to_right else range(n - 1)
        for o in order:
            beyond = o > z if to_right else o < z
            at = part(c, o)

            @pl.when(jnp.logical_and(beyond, first))
            def _():
                acc[at] = encode(step_ref[at])
                send_sum(acc, c, o, to_right).start()

            @pl.when(jnp.logical_and(beyond, jnp.logical_not(first)))
            def _():
                send_sum(acc, c, o, to_right).wait_recv()
                came = (from_left if to_right else from_right)[at]
                acc[at] = encode(decode(came) + step_ref[at])
                send_sum(acc, c, o, to_right).start()

    def own(c):
        at = part(c, z)
        here = pl.ds(pl.multiple_of(c * rc, rc), rc)
        total[...] = step_ref[at]

        @pl.when(has_left)
        def _():
            send_sum(acc, c, z, True).wait_recv()
            total[...] += decode(from_left[at])

        @pl.when(has_right)
        def _():
            send_sum(acc, c, z, False).wait_recv()
            total[...] += decode(from_right[at])

        delta = outer_ref[here, :] - total[...] / n
        momentum = nesterov * mom_ref[here, :] + delta
        newmom_ref[here, :] = momentum
        updated = outer_ref[here, :] - outer_rate * (delta + nesterov * momentum)
        out_ref[at] = updated.astype(WIRE)

        @pl.when(has_right)
        def _():
            send_new(c, z, True).start()

        @pl.when(has_left)
        def _():
            send_new(c, z, False).start()

    def within(c, work):
        @pl.when(jnp.logical_and(c >= 0, c < chunks))
        def _():
            work(c)

    def own_lag(o):
        return jnp.maximum(o, n - 1 - o)

    def forward(t, distance, to_right):
        o = z - distance if to_right else z + distance
        there = o >= 0 if to_right else o < n
        c = t - own_lag(o) - distance
        ready = jnp.logical_and(there, jnp.logical_and(c >= 0, c < chunks))

        @pl.when(ready)
        def _():
            send_new(c, o, to_right).wait_recv()

        @pl.when(jnp.logical_and(ready, has_right if to_right else has_left))
        def _():
            send_new(c, o, to_right).start()

    def body(t, carry):
        within(t - z, lambda c: wave(c, True))
        within(t - (n - 1 - z), lambda c: wave(c, False))
        within(t - own_lag(z), own)
        for distance in range(1, n):
            forward(t, distance, True)
            forward(t, distance, False)
        return carry

    lax.fori_loop(0, chunks + 2 * (n - 1), body, 0)

    def drain(c, carry):
        for o in range(n):
            @pl.when(o > z)
            def _():
                send_sum(acc, c, o, True).wait_send()

            @pl.when(o < z)
            def _():
                send_sum(acc, c, o, False).wait_send()

            @pl.when(jnp.logical_and(o <= z, has_right))
            def _():
                send_new(c, o, True).wait_send()

            @pl.when(jnp.logical_and(o >= z, has_left))
            def _():
                send_new(c, o, False).wait_send()

        return carry

    lax.fori_loop(0, chunks, drain, 0)


def outer_step(stepped, outer_params, outer_momentum):
    n = lax.axis_size("rep")
    rows, block = outer_params.shape
    chunks = max(c for c in range(1, 15) if rows % (16 * c) == 0)
    vmem = pl.BlockSpec(memory_space=pltpu.VMEM)
    dma = pltpu.SemaphoreType.DMA((chunks, n))
    return pl.pallas_call(
        functools.partial(outer_kernel, n, chunks),
        out_shape=(
            jax.ShapeDtypeStruct(stepped.shape, WIRE),
            jax.ShapeDtypeStruct(outer_params.shape, jnp.float32),
        ),
        in_specs=[vmem] * 3,
        out_specs=(vmem, vmem),
        scratch_shapes=[
            pltpu.VMEM(stepped.shape, WIRE),
            pltpu.VMEM(stepped.shape, WIRE),
            pltpu.VMEM(stepped.shape, WIRE),
            pltpu.VMEM((rows // chunks, block), jnp.float32),
            dma, dma, dma, dma, dma, dma,
        ],
        compiler_params=pltpu.CompilerParams(
            collective_id=0, has_side_effects=True, vmem_limit_bytes=40 * 2**20
        ),
    )(stepped, outer_params, outer_momentum)


ROW_TILE = 128
COL_TILE = 256
HOP_STEPS = 3
AHEAD = 2
SHELL_STEPS = 8
CODE_RANGE = 560.0


def fused_kernel(
    cfg,
    hid, og, par_hbm, first_hbm, second_hbm, outer_hbm, mom_hbm,
    out_ref, newmom_ref, newfirst_ref, newsecond_ref,
    hbuf, ht, obuf, step, first, second, outer, mom, acc, from_left, from_right,
    h_send, h_recv, o_send, o_recv, sib_send, sib_recv, load_sem,
    left_sem, right_sem, gather_sem, rs_send, ag_right, ag_left,
):
    n, peers, rows, width, tokens = cfg
    ni, nj = rows // ROW_TILE, width // COL_TILE
    stages = max(ni, nj)
    halves = nj // n
    chips = peers // 2
    z = lax.axis_index("rep")
    me = lax.axis_index("fsdp")
    core, chip = me % 2, me // 2
    has_left, has_right = z > 0, z < n - 1

    def flag(condition):
        return condition.astype(jnp.int32)

    def peer_chip(d):
        return ((chip // 2 + d // 2) % (chips // 2)) * 2 + (chip + d) % 2

    sibling = chip * 2 + 1 - core

    barrier = pltpu.get_barrier_semaphore()
    for d in range(1, peers):
        target = peer_chip(d // 2) * 2 + (core + d) % 2
        pl.semaphore_signal(barrier, inc=1, device_id={"fsdp": target})

    @pl.when(has_left)
    def _():
        pl.semaphore_signal(barrier, inc=1, device_id={"rep": z - 1})

    @pl.when(has_right)
    def _():
        pl.semaphore_signal(barrier, inc=1, device_id={"rep": z + 1})

    pl.semaphore_wait(barrier, peers - 1 + flag(has_left) + flag(has_right))

    counts = [
        (ni if s >= ni else nj if s >= nj else 2 * s + 1) for s in range(stages)
    ]
    widths = [max(c, SHELL_STEPS) if s < stages - 1 else c for s, c in enumerate(counts)]
    starts = [sum(widths[:s]) for s in range(stages + 1)]
    total_steps = starts[-1]

    def chunk_of(j):
        return (j + (n - 1) * halves) % nj

    def own_lag(o):
        return max(o, n - 1 - o) if isinstance(o, int) else jnp.maximum(o, n - 1 - o)

    def place(u):
        s = jnp.int32(0)
        base = jnp.int32(0)
        for a, b in zip(starts[:-2], starts[1:-1]):
            past = flag(u >= b)
            s = s + past
            base = base + past * (b - a)
        return s, u - base

    def tile(u):
        s, q = place(u)
        low = q < s
        i = jnp.where(low, q, s)
        j = jnp.where(low, s, q - s)
        count = jnp.where(s >= ni, ni, 2 * s + 1)
        valid = (u >= 0) & (u < total_steps) & (q < count)
        return valid, i, j, chunk_of(j)

    def rows_of(i):
        return pl.ds(pl.multiple_of(i * ROW_TILE, ROW_TILE), ROW_TILE)

    def cols_of(c):
        return pl.ds(pl.multiple_of(c * COL_TILE, COL_TILE), COL_TILE)

    def hid_cols(owner, s):
        return pl.ds(pl.multiple_of(owner * rows + s * ROW_TILE, ROW_TILE), ROW_TILE)

    def send_o(s, d):
        return pltpu.make_async_remote_copy(
            src_ref=og.at[:, cols_of(chunk_of(s))],
            dst_ref=obuf.at[s, me],
            send_sem=o_send.at[s],
            recv_sem=o_recv.at[s, chip],
            device_id={"fsdp": peer_chip(d) * 2 + core},
        )

    def issue_o(s):
        for d in range(1, chips):
            send_o(s, d).start()
        pltpu.make_async_remote_copy(
            src_ref=og.at[:, cols_of(chunk_of(s))],
            dst_ref=obuf.at[s, me],
            send_sem=sib_send.at[s],
            recv_sem=sib_recv.at[s],
            device_id={"fsdp": sibling},
        ).start()
        pltpu.make_async_copy(
            og.at[:, cols_of(chunk_of(s))], obuf.at[s, me], o_recv.at[s, chip]
        ).start()

    def forward_o(s):
        for d in range(chips):
            source = peer_chip(d)
            block = source * 2 + core
            pltpu.make_async_copy(
                obuf.at[s, block], obuf.at[s, block], o_recv.at[s, source]
            ).wait()
            if d > 0:
                pltpu.make_async_remote_copy(
                    src_ref=obuf.at[s, block],
                    dst_ref=obuf.at[s, block],
                    send_sem=sib_send.at[s],
                    recv_sem=sib_recv.at[s],
                    device_id={"fsdp": sibling},
                ).start()

    def issue_h(s):
        for d in list(range(2, peers)) + [1]:
            target = peer_chip(d // 2) * 2 + (core + d) % 2
            pltpu.make_async_remote_copy(
                src_ref=hid.at[:, hid_cols(target, s)],
                dst_ref=hbuf.at[s, me],
                send_sem=h_send.at[s],
                recv_sem=h_recv.at[s],
                device_id={"fsdp": target},
            ).start()
        pltpu.make_async_copy(
            hid.at[:, hid_cols(me, s)], hbuf.at[s, me], h_recv.at[s]
        ).start()

    def issue(s):
        if isinstance(s, int):
            if s < nj:
                issue_o(s)
            if s < ni:
                issue_h(s)
        else:
            @pl.when(s < nj)
            def _():
                issue_o(s)

            @pl.when(s < ni)
            def _():
                issue_h(s)

    for s in range(AHEAD):
        issue(s)
    loads = [
        pltpu.make_async_copy(a, b, load_sem.at[k])
        for k, (a, b) in enumerate(
            ((par_hbm, step), (first_hbm, first), (second_hbm, second), (outer_hbm, outer), (mom_hbm, mom))
        )
    ]
    for load in loads:
        load.start()

    def code_scale(terms):
        return CODE_RANGE / terms.astype(jnp.float32)

    def encode(value, terms):
        return jnp.exp(value * code_scale(terms)).astype(WIRE)

    def decode(coded, terms):
        return jnp.log(coded.astype(jnp.float32)) * (1.0 / code_scale(terms))

    def send_sum(i, j, o, to_right):
        return pltpu.make_async_remote_copy(
            src_ref=acc.at[i, j],
            dst_ref=(from_left if to_right else from_right).at[i, j],
            send_sem=rs_send.at[o],
            recv_sem=(left_sem if to_right else right_sem).at[i, j],
            device_id={"rep": z + 1 if to_right else z - 1},
        )

    def send_new(i, j, c, to_right):
        at = rows_of(i), cols_of(c)
        return pltpu.make_async_remote_copy(
            src_ref=out_ref.at[at],
            dst_ref=out_ref.at[at],
            send_sem=(ag_right if to_right else ag_left).at[c // halves],
            recv_sem=gather_sem.at[i, j],
            device_id={"rep": z + 1 if to_right else z - 1},
        )

    def wave(t, to_right):
        hop = z if to_right else n - 1 - z
        valid, i, j, c = tile(t - hop * HOP_STEPS)
        o = c // halves
        beyond = (o > z) if to_right else (o < z)
        at = rows_of(i), cols_of(c)
        active = valid & beyond

        @pl.when(active & (hop == 0))
        def _():
            acc[i, j] = encode(step[at], hop + 1)
            send_sum(i, j, o, to_right).start()

        @pl.when(active & (hop > 0))
        def _():
            send_sum(i, j, o, to_right).wait_recv()
            came = (from_left if to_right else from_right)[i, j]
            acc[i, j] = encode(decode(came, hop) + step[at], hop + 1)
            send_sum(i, j, o, to_right).start()

    def own(t):
        valid, i, j, c = tile(t - own_lag(z) * HOP_STEPS)

        @pl.when(valid & (c // halves == z))
        def _():
            at = rows_of(i), cols_of(c)
            local = rows_of(i), cols_of(c % halves)

            @pl.when(has_left)
            def _():
                send_sum(i, j, z, True).wait_recv()
                step[at] += decode(from_left[i, j], z)

            @pl.when(has_right)
            def _():
                send_sum(i, j, z, False).wait_recv()
                step[at] += decode(from_right[i, j], n - 1 - z)

            delta = outer[local] - step[at] * (1.0 / n)
            momentum = nesterov * mom[local] + delta
            newmom_ref[local] = momentum
            updated = outer[local] - outer_rate * (delta + nesterov * momentum)
            out_ref[at] = updated.astype(WIRE)

            @pl.when(has_right)
            def _():
                send_new(i, j, c, True).start()

            @pl.when(has_left)
            def _():
                send_new(i, j, c, False).start()

    def pass_on(t, e):
        o = (z + e) % n
        to_right = o < z
        distance = jnp.where(to_right, z - o, o - z)
        valid, i, j, c = tile(t - (own_lag(o) + distance) * HOP_STEPS)
        ready = valid & (c // halves == o)

        @pl.when(ready)
        def _():
            send_new(i, j, c, True).wait_recv()

            @pl.when(to_right & has_right)
            def _():
                send_new(i, j, c, True).start()

            @pl.when((o > z) & has_left)
            def _():
                send_new(i, j, c, False).start()

    def compute(t):
        s, q = place(t)
        valid, i, j, c = tile(t)

        @pl.when((q == 0) & (t < total_steps))
        def _():
            issue(s + AHEAD)

            @pl.when(s < ni)
            def _():
                pltpu.make_async_copy(hbuf.at[s], hbuf.at[s], h_recv.at[s]).wait()
                ht[s] = hbuf[s].reshape(peers * tokens, ROW_TILE).T

            @pl.when(s < nj)
            def _():
                four = obuf.at[s, pl.ds(0, chips)]
                pltpu.make_async_copy(four, four, sib_recv.at[s]).wait()

        @pl.when((q == SHELL_STEPS // 2) & (s + 1 < nj) & (t < total_steps))
        def _():
            forward_o(s + 1)

        @pl.when(valid)
        def _():
            at = rows_of(i), cols_of(c)
            gradient = jnp.dot(
                ht[i],
                obuf[j].reshape(peers * tokens, COL_TILE),
                preferred_element_type=jnp.float32,
            )
            one = beta_one * first[at].astype(jnp.float32) + (1.0 - beta_one) * gradient
            two = beta_two * second[at].astype(jnp.float32) + (1.0 - beta_two) * gradient * gradient
            newfirst_ref[at] = one.astype(jnp.bfloat16)
            newsecond_ref[at] = two.astype(jnp.bfloat16)
            corrected_one = one * (1.0 / (1.0 - beta_one**INNER_STEP))
            corrected_two = two * (1.0 / (1.0 - beta_two**INNER_STEP))
            held = step[at]
            step[at] = held - inner_rate * (
                corrected_one / (jnp.sqrt(corrected_two) + epsilon) + weight_decay * held
            )

    forward_o(0)
    for load in loads:
        load.wait()

    last = 0
    for s, c in enumerate(counts):
        for q in range(c):
            j = q if s >= nj else (s if q < s else q - s)
            o = ((j + (n - 1) * halves) % nj) // halves
            lag = own_lag(o) + max(o, n - 1 - o)
            last = max(last, starts[s] + q + lag * HOP_STEPS)

    def body(t, carry):
        for e in range(1, n):
            pass_on(t, e)
        own(t)
        compute(t)
        wave(t, True)
        wave(t, False)
        return carry

    lax.fori_loop(0, last + 1, body, 0)

    for o in range(n):
        part = acc.at[:, pl.ds(0, halves)]

        @pl.when(z != o)
        def _():
            pltpu.make_async_copy(part, part, rs_send.at[o]).wait()

        @pl.when((o <= z) & has_right)
        def _():
            pltpu.make_async_copy(part, part, ag_right.at[o]).wait()

        @pl.when((o >= z) & has_left)
        def _():
            pltpu.make_async_copy(part, part, ag_left.at[o]).wait()

    for s in range(ni):
        sent = hbuf.at[s, pl.ds(0, peers - 1)]
        pltpu.make_async_copy(sent, sent, h_send.at[s]).wait()
    for s in range(nj):
        sent = obuf.at[s, pl.ds(0, chips - 1)]
        pltpu.make_async_copy(sent, sent, o_send.at[s]).wait()
        sent = obuf.at[s, pl.ds(0, chips)]
        pltpu.make_async_copy(sent, sent, sib_send.at[s]).wait()


def fused(hidden, out_grad, inner_params, first_moment, second_moment, outer_params, outer_momentum):
    n, peers = lax.axis_size("rep"), lax.axis_size("fsdp")
    tokens = hidden.shape[0]
    rows, width = inner_params.shape
    block = outer_params.shape[1]
    ni, nj = rows // ROW_TILE, width // COL_TILE
    cfg = (n, peers, rows, width, tokens)
    anywhere = pl.BlockSpec(memory_space=pl.ANY)
    vmem = pl.BlockSpec(memory_space=pltpu.VMEM)
    dma = pltpu.SemaphoreType.DMA
    bf16, f32 = jnp.bfloat16, jnp.float32
    return pl.pallas_call(
        functools.partial(fused_kernel, cfg),
        out_shape=(
            jax.ShapeDtypeStruct((rows, width), WIRE),
            jax.ShapeDtypeStruct((rows, block), f32),
            jax.ShapeDtypeStruct((rows, width), bf16),
            jax.ShapeDtypeStruct((rows, width), bf16),
        ),
        in_specs=[anywhere] * 7,
        out_specs=(vmem,) * 4,
        scratch_shapes=[
            pltpu.VMEM((ni, peers, tokens, ROW_TILE), bf16),
            pltpu.VMEM((ni, ROW_TILE, peers * tokens), bf16),
            pltpu.VMEM((nj, peers, tokens, COL_TILE), bf16),
            pltpu.VMEM((rows, width), f32),
            pltpu.VMEM((rows, width), bf16),
            pltpu.VMEM((rows, width), bf16),
            pltpu.VMEM((rows, block), f32),
            pltpu.VMEM((rows, block), f32),
            pltpu.VMEM((ni, nj, ROW_TILE, COL_TILE), WIRE),
            pltpu.VMEM((ni, nj, ROW_TILE, COL_TILE), WIRE),
            pltpu.VMEM((ni, nj, ROW_TILE, COL_TILE), WIRE),
            dma((ni,)), dma((ni,)),
            dma((nj,)), dma((nj, peers // 2)), dma((nj,)), dma((nj,)), dma((5,)),
            dma((ni, nj)), dma((ni, nj)), dma((ni, nj)),
            dma((n,)), dma((n,)), dma((n,)),
        ],
        compiler_params=pltpu.CompilerParams(
            collective_id=1, has_side_effects=True, vmem_limit_bytes=67043328
        ),
    )(hidden, out_grad, inner_params, first_moment, second_moment, outer_params, outer_momentum)


def fits(peers, n, rows, width, block, tokens):
    if peers % 4 or rows % ROW_TILE or block % COL_TILE or tokens % 16:
        return False
    return rows // ROW_TILE <= width // COL_TILE


def per_device(
    hidden, out_grad, inner_params, first_moment, second_moment, outer_params, outer_momentum
):
    rows, width = inner_params.shape[1:]
    block, tokens = outer_params.shape[1], hidden.shape[0]
    if fits(lax.axis_size("fsdp"), lax.axis_size("rep"), rows, width, block, tokens):
        gathered, new_momentum, new_first, new_second = fused(
            hidden, out_grad, inner_params[0], first_moment[0], second_moment[0],
            outer_params, outer_momentum,
        )
        return gathered.astype(jnp.float32), new_momentum, new_first[None], new_second[None]
    columns = lax.all_to_all(hidden, "fsdp", split_axis=1, concat_axis=0, tiled=True)
    segment = lax.all_gather(out_grad, "fsdp", axis=0, tiled=True)
    token_count = hidden.shape[0]
    blocks = segment.shape[0] // token_count
    gradient = jnp.einsum(
        "btf,btd->fd",
        columns.reshape(blocks, token_count, columns.shape[1]),
        segment.reshape(blocks, token_count, segment.shape[1]),
        preferred_element_type=jnp.float32,
    )
    stacked = gradient[None]
    moment_one = beta_one * first_moment.astype(jnp.float32) + (1.0 - beta_one) * stacked
    moment_two = beta_two * second_moment.astype(jnp.float32) + (1.0 - beta_two) * stacked * stacked
    corrected_one = moment_one / (1.0 - beta_one**INNER_STEP)
    corrected_two = moment_two / (1.0 - beta_two**INNER_STEP)
    stepped = inner_params - inner_rate * (
        corrected_one / (jnp.sqrt(corrected_two) + epsilon) + weight_decay * inner_params
    )
    gathered, new_momentum = outer_step(stepped[0], outer_params, outer_momentum)
    return (
        gathered.astype(jnp.float32),
        new_momentum,
        moment_one.astype(jnp.bfloat16),
        moment_two.astype(jnp.bfloat16),
    )


def solution(mesh):
    return jax.shard_map(
        per_device,
        mesh=mesh,
        in_specs=(
            P(("rep", "fsdp"), None),
            P(("rep", "fsdp"), None),
            P("rep", "fsdp", None),
            P("rep", "fsdp", None),
            P("rep", "fsdp", None),
            P("fsdp", "rep"),
            P("fsdp", "rep"),
        ),
        out_specs=(
            P("fsdp", None),
            P("fsdp", "rep"),
            P("rep", "fsdp", None),
            P("rep", "fsdp", None),
        ),
        check_vma=False,
    )
```

```python
import functools

import jax
import jax.numpy as jnp
from jax import lax
from jax.experimental import pallas as pl
from jax.experimental.pallas import tpu as pltpu
from jax.sharding import PartitionSpec as P

INNER_STEP = 500

beta_one = 0.9
beta_two = 0.95
epsilon = 1e-08
inner_rate = 0.0004
weight_decay = 0.1
outer_rate = 0.7
nesterov = 0.9

WIRE = jnp.bfloat16
WIRE_SCALE = 16.0


def encode(value):
    scaled = value * WIRE_SCALE
    square = scaled * scaled
    fourth = square * square
    eighth = fourth * fourth
    return jnp.where(scaled < 0.0, -eighth, eighth).astype(WIRE)


def decode(coded):
    wide = coded.astype(jnp.float32)
    root = jnp.sqrt(jnp.sqrt(jnp.sqrt(jnp.abs(wide)))) * (1.0 / WIRE_SCALE)
    return jnp.where(wide < 0.0, -root, root)


def outer_kernel(
    n, chunks, step_ref, outer_ref, mom_ref, out_ref, newmom_ref,
    from_left, from_right, acc, total,
    rs_send, rs_left, rs_right, ag_right, ag_left, ag_recv,
):
    z = lax.axis_index("rep")
    rows, block = outer_ref.shape
    rc = rows // chunks
    has_left, has_right = z > 0, z < n - 1

    barrier = pltpu.get_barrier_semaphore()

    @pl.when(has_left)
    def _():
        pl.semaphore_signal(barrier, inc=1, device_id={"rep": z - 1})

    @pl.when(has_right)
    def _():
        pl.semaphore_signal(barrier, inc=1, device_id={"rep": z + 1})

    pl.semaphore_wait(barrier, has_left.astype(jnp.int32) + has_right.astype(jnp.int32))

    def part(c, o):
        start = o * block
        if not isinstance(o, int):
            start = pl.multiple_of(start, 128)
        return pl.ds(pl.multiple_of(c * rc, rc), rc), pl.ds(start, block)

    def send_sum(src, c, o, to_right):
        at = part(c, o)
        return pltpu.make_async_remote_copy(
            src_ref=src.at[at],
            dst_ref=(from_left if to_right else from_right).at[at],
            send_sem=rs_send.at[c, o],
            recv_sem=(rs_left if to_right else rs_right).at[c, o],
            device_id={"rep": z + 1 if to_right else z - 1},
        )

    def send_new(c, o, to_right):
        at = part(c, o)
        return pltpu.make_async_remote_copy(
            src_ref=out_ref.at[at],
            dst_ref=out_ref.at[at],
            send_sem=(ag_right if to_right else ag_left).at[c, o],
            recv_sem=ag_recv.at[c, o],
            device_id={"rep": z + 1 if to_right else z - 1},
        )

    def wave(c, to_right):
        first = z == 0 if to_right else z == n - 1
        order = range(n - 1, 0, -1) if to_right else range(n - 1)
        for o in order:
            beyond = o > z if to_right else o < z
            at = part(c, o)

            @pl.when(jnp.logical_and(beyond, first))
            def _():
                acc[at] = encode(step_ref[at])
                send_sum(acc, c, o, to_right).start()

            @pl.when(jnp.logical_and(beyond, jnp.logical_not(first)))
            def _():
                send_sum(acc, c, o, to_right).wait_recv()
                came = (from_left if to_right else from_right)[at]
                acc[at] = encode(decode(came) + step_ref[at])
                send_sum(acc, c, o, to_right).start()

    def own(c):
        at = part(c, z)
        here = pl.ds(pl.multiple_of(c * rc, rc), rc)
        total[...] = step_ref[at]

        @pl.when(has_left)
        def _():
            send_sum(acc, c, z, True).wait_recv()
            total[...] += decode(from_left[at])

        @pl.when(has_right)
        def _():
            send_sum(acc, c, z, False).wait_recv()
            total[...] += decode(from_right[at])

        delta = outer_ref[here, :] - total[...] / n
        momentum = nesterov * mom_ref[here, :] + delta
        newmom_ref[here, :] = momentum
        updated = outer_ref[here, :] - outer_rate * (delta + nesterov * momentum)
        out_ref[at] = updated.astype(WIRE)

        @pl.when(has_right)
        def _():
            send_new(c, z, True).start()

        @pl.when(has_left)
        def _():
            send_new(c, z, False).start()

    def within(c, work):
        @pl.when(jnp.logical_and(c >= 0, c < chunks))
        def _():
            work(c)

    def own_lag(o):
        return jnp.maximum(o, n - 1 - o)

    def forward(t, distance, to_right):
        o = z - distance if to_right else z + distance
        there = o >= 0 if to_right else o < n
        c = t - own_lag(o) - distance
        ready = jnp.logical_and(there, jnp.logical_and(c >= 0, c < chunks))

        @pl.when(ready)
        def _():
            send_new(c, o, to_right).wait_recv()

        @pl.when(jnp.logical_and(ready, has_right if to_right else has_left))
        def _():
            send_new(c, o, to_right).start()

    def body(t, carry):
        within(t - z, lambda c: wave(c, True))
        within(t - (n - 1 - z), lambda c: wave(c, False))
        within(t - own_lag(z), own)
        for distance in range(1, n):
            forward(t, distance, True)
            forward(t, distance, False)
        return carry

    lax.fori_loop(0, chunks + 2 * (n - 1), body, 0)

    def drain(c, carry):
        for o in range(n):
            @pl.when(o > z)
            def _():
                send_sum(acc, c, o, True).wait_send()

            @pl.when(o < z)
            def _():
                send_sum(acc, c, o, False).wait_send()

            @pl.when(jnp.logical_and(o <= z, has_right))
            def _():
                send_new(c, o, True).wait_send()

            @pl.when(jnp.logical_and(o >= z, has_left))
            def _():
                send_new(c, o, False).wait_send()

        return carry

    lax.fori_loop(0, chunks, drain, 0)


def outer_step(stepped, outer_params, outer_momentum):
    n = lax.axis_size("rep")
    rows, block = outer_params.shape
    chunks = max(c for c in range(1, 15) if rows % (16 * c) == 0)
    vmem = pl.BlockSpec(memory_space=pltpu.VMEM)
    dma = pltpu.SemaphoreType.DMA((chunks, n))
    return pl.pallas_call(
        functools.partial(outer_kernel, n, chunks),
        out_shape=(
            jax.ShapeDtypeStruct(stepped.shape, WIRE),
            jax.ShapeDtypeStruct(outer_params.shape, jnp.float32),
        ),
        in_specs=[vmem] * 3,
        out_specs=(vmem, vmem),
        scratch_shapes=[
            pltpu.VMEM(stepped.shape, WIRE),
            pltpu.VMEM(stepped.shape, WIRE),
            pltpu.VMEM(stepped.shape, WIRE),
            pltpu.VMEM((rows // chunks, block), jnp.float32),
            dma, dma, dma, dma, dma, dma,
        ],
        compiler_params=pltpu.CompilerParams(
            collective_id=0, has_side_effects=True, vmem_limit_bytes=40 * 2**20
        ),
    )(stepped, outer_params, outer_momentum)


ROW_TILE = 128
VMEM_BYTES = 40000000
COL_TILE = 256
HOP_STEPS = 5
AHEAD = 2
SEGMENT_STEPS = 6
LEAD = 1
EDGE_LAG = 3
CODE_RANGE = 560.0


def fused_kernel(
    cfg,
    hid, og, par_hbm, first_hbm, second_hbm, outer_hbm, mom_hbm,
    wide_ref, mom, first, second,
    hbuf, ht, obuf, step, outer, out_ref, from_left, from_right,
    h_send, h_recv, o_send, o_recv, sib_send, sib_recv, load_sem,
    left_sem, right_sem, gather_sem, rs_send, ag_right, ag_left,
):
    n, peers, rows, width, tokens = cfg
    ni, nj = rows // ROW_TILE, width // COL_TILE
    stages = max(ni, nj)
    halves = nj // n
    chips = peers // 2
    z = lax.axis_index("rep")
    me = lax.axis_index("fsdp")
    core, chip = me % 2, me // 2
    has_left, has_right = z > 0, z < n - 1

    def flag(condition):
        return condition.astype(jnp.int32)

    def peer_chip(d):
        return ((chip // 2 + d // 2) % (chips // 2)) * 2 + (chip + d) % 2

    sibling = chip * 2 + 1 - core

    barrier = pltpu.get_barrier_semaphore()
    for d in range(1, peers):
        target = peer_chip(d // 2) * 2 + (core + d) % 2
        pl.semaphore_signal(barrier, inc=1, device_id={"fsdp": target})

    @pl.when(has_left)
    def _():
        pl.semaphore_signal(barrier, inc=1, device_id={"rep": z - 1})

    @pl.when(has_right)
    def _():
        pl.semaphore_signal(barrier, inc=1, device_id={"rep": z + 1})

    pl.semaphore_wait(barrier, peers - 1 + flag(has_left) + flag(has_right))

    segments = ni + nj - 1
    counts = [(g + 2) // 2 for g in range(segments)]
    leads = [LEAD * (g % 2) for g in range(segments)]
    widths = [
        max(c + a, SEGMENT_STEPS) if g < segments - 1 else c + a
        for g, (c, a) in enumerate(zip(counts, leads))
    ]
    starts = [sum(widths[:g]) for g in range(segments + 1)]
    total_steps = starts[-1]

    def chunk_of(j):
        return (j + (n - 1) * halves) % nj

    def own_lag(o):
        return max(o, n - 1 - o) if isinstance(o, int) else jnp.maximum(o, n - 1 - o)

    def place(u):
        g = jnp.int32(0)
        base = jnp.int32(0)
        for a, b in zip(starts[:-2], starts[1:-1]):
            past = flag(u >= b)
            g = g + past
            base = base + past * (b - a)
        return g, u - base

    def tile(u):
        g, q = place(u)
        odd = g % 2
        half = (g + 1) // 2
        q = q - LEAD * odd
        i = jnp.where(odd == 1, q, half)
        j = jnp.where(odd == 1, half, q)
        valid = (u >= 0) & (u < total_steps) & (q >= 0) & (q < half + 1 - odd)
        return valid, i, j, chunk_of(j)

    def rows_of(i):
        return pl.ds(pl.multiple_of(i * ROW_TILE, ROW_TILE), ROW_TILE)

    def cols_of(c):
        return pl.ds(pl.multiple_of(c * COL_TILE, COL_TILE), COL_TILE)

    def hid_cols(owner, s):
        return pl.ds(pl.multiple_of(owner * rows + s * ROW_TILE, ROW_TILE), ROW_TILE)

    def send_o(s, d):
        return pltpu.make_async_remote_copy(
            src_ref=og.at[:, cols_of(chunk_of(s))],
            dst_ref=obuf.at[s, me],
            send_sem=o_send.at[s],
            recv_sem=o_recv.at[s, chip],
            device_id={"fsdp": peer_chip(d) * 2 + core},
        )

    def issue_o(s):
        for d in range(1, chips):
            send_o(s, d).start()
        pltpu.make_async_remote_copy(
            src_ref=og.at[:, cols_of(chunk_of(s))],
            dst_ref=obuf.at[s, me],
            send_sem=sib_send.at[s],
            recv_sem=sib_recv.at[s],
            device_id={"fsdp": sibling},
        ).start()
        pltpu.make_async_copy(
            og.at[:, cols_of(chunk_of(s))], obuf.at[s, me], o_recv.at[s, chip]
        ).start()

    def forward_o(s):
        for d in range(chips):
            source = peer_chip(d)
            block = source * 2 + core
            pltpu.make_async_copy(
                obuf.at[s, block], obuf.at[s, block], o_recv.at[s, source]
            ).wait()
            if d > 0:
                pltpu.make_async_remote_copy(
                    src_ref=obuf.at[s, block],
                    dst_ref=obuf.at[s, block],
                    send_sem=sib_send.at[s],
                    recv_sem=sib_recv.at[s],
                    device_id={"fsdp": sibling},
                ).start()

    def gathered_o(s):
        four = obuf.at[s, pl.ds(0, chips)]
        pltpu.make_async_copy(four, four, sib_recv.at[s]).wait()

    def issue_h(s):
        for d in list(range(2, peers)) + [1]:
            target = peer_chip(d // 2) * 2 + (core + d) % 2
            pltpu.make_async_remote_copy(
                src_ref=hid.at[:, hid_cols(target, s)],
                dst_ref=hbuf.at[s, me],
                send_sem=h_send.at[s],
                recv_sem=h_recv.at[s],
                device_id={"fsdp": target},
            ).start()
        pltpu.make_async_copy(
            hid.at[:, hid_cols(me, s)], hbuf.at[s, me], h_recv.at[s]
        ).start()

    def issue(s):
        if isinstance(s, int):
            if s < nj:
                issue_o(s)
            if s < ni:
                issue_h(s)
        else:
            @pl.when(s < nj)
            def _():
                issue_o(s)

            @pl.when(s < ni)
            def _():
                issue_h(s)

    for s in range(AHEAD):
        issue(s)
    loads = [
        pltpu.make_async_copy(a, b, load_sem.at[k])
        for k, (a, b) in enumerate(
            ((par_hbm, step), (first_hbm, first), (second_hbm, second), (outer_hbm, outer), (mom_hbm, mom))
        )
    ]
    for load in loads:
        load.start()

    def code_scale(terms):
        return CODE_RANGE / terms.astype(jnp.float32)

    def encode(value, terms):
        return jnp.exp(value * code_scale(terms)).astype(WIRE)

    def decode(coded, terms):
        return jnp.log(coded.astype(jnp.float32)) * (1.0 / code_scale(terms))

    def send_sum(i, j, o, to_right):
        return pltpu.make_async_remote_copy(
            src_ref=(from_left if to_right else from_right).at[i, j],
            dst_ref=(from_left if to_right else from_right).at[i, j],
            send_sem=rs_send.at[o],
            recv_sem=(left_sem if to_right else right_sem).at[i, j],
            device_id={"rep": z + 1 if to_right else z - 1},
        )

    def send_new(i, j, c, to_right):
        at = rows_of(i), cols_of(c)
        return pltpu.make_async_remote_copy(
            src_ref=out_ref.at[at],
            dst_ref=out_ref.at[at],
            send_sem=(ag_right if to_right else ag_left).at[c // halves],
            recv_sem=gather_sem.at[i, j],
            device_id={"rep": z + 1 if to_right else z - 1},
        )

    def wave(t, to_right):
        hop = z if to_right else n - 1 - z
        valid, i, j, c = tile(t - hop * HOP_STEPS)
        o = c // halves
        beyond = (o > z) if to_right else (o < z)
        at = rows_of(i), cols_of(c)
        active = valid & beyond
        partial = from_left if to_right else from_right

        @pl.when(active & (hop == 0))
        def _():
            partial[i, j] = encode(step[at], hop + 1)
            send_sum(i, j, o, to_right).start()

        @pl.when(active & (hop > 0))
        def _():
            send_sum(i, j, o, to_right).wait_recv()
            partial[i, j] = encode(decode(partial[i, j], hop) + step[at], hop + 1)
            send_sum(i, j, o, to_right).start()

    def own(t):
        valid, i, j, c = tile(t - own_lag(z) * HOP_STEPS)

        @pl.when(valid & (c // halves == z))
        def _():
            at = rows_of(i), cols_of(c)
            local = rows_of(i), cols_of(c % halves)

            @pl.when(has_left)
            def _():
                send_sum(i, j, z, True).wait_recv()
                step[at] += decode(from_left[i, j], z)

            @pl.when(has_right)
            def _():
                send_sum(i, j, z, False).wait_recv()
                step[at] += decode(from_right[i, j], n - 1 - z)

            delta = outer[local] - step[at] * (1.0 / n)
            momentum = nesterov * mom[local] + delta
            mom[local] = momentum
            updated = outer[local] - outer_rate * (delta + nesterov * momentum)
            out_ref[at] = updated.astype(WIRE)
            wide_ref[at] = updated

            @pl.when(has_right)
            def _():
                send_new(i, j, c, True).start()

            @pl.when(has_left)
            def _():
                send_new(i, j, c, False).start()

    def pass_on(t, e):
        o = (z + e) % n
        to_right = o < z
        distance = jnp.where(to_right, z - o, o - z)
        edge = jnp.where(to_right, flag(has_right), flag(has_left)) == 0
        lag = (own_lag(o) + distance) * HOP_STEPS + EDGE_LAG * flag(edge)
        valid, i, j, c = tile(t - lag)
        ready = valid & (c // halves == o)
        at = rows_of(i), cols_of(c)

        @pl.when(ready)
        def _():
            send_new(i, j, c, True).wait_recv()

            @pl.when(to_right & has_right)
            def _():
                send_new(i, j, c, True).start()

            @pl.when((o > z) & has_left)
            def _():
                send_new(i, j, c, False).start()

            wide_ref[at] = out_ref[at].astype(jnp.float32)

    def compute(t):
        g, q = place(t)
        s = (g + 1) // 2
        inside = t < total_steps
        valid, i, j, c = tile(t)

        @pl.when(inside & (g % 2 == 0) & (q == 0))
        def _():
            issue(s + AHEAD)
            pltpu.make_async_copy(hbuf.at[s], hbuf.at[s], h_recv.at[s]).wait()
            ht[s] = hbuf[s].reshape(peers * tokens, ROW_TILE).T

        @pl.when(inside & (g % 2 == 1) & (q == 0))
        def _():
            forward_o(s)

        @pl.when(inside & (g % 2 == 1) & (q == LEAD))
        def _():
            gathered_o(s)

        @pl.when(valid)
        def _():
            at = rows_of(i), cols_of(c)
            gradient = jnp.dot(
                ht[i],
                obuf[j].reshape(peers * tokens, COL_TILE),
                preferred_element_type=jnp.float32,
            )
            one = beta_one * first[at].astype(jnp.float32) + (1.0 - beta_one) * gradient
            two = beta_two * second[at].astype(jnp.float32) + (1.0 - beta_two) * gradient * gradient
            first[at] = one.astype(jnp.bfloat16)
            second[at] = two.astype(jnp.bfloat16)
            corrected_one = one * (1.0 / (1.0 - beta_one**INNER_STEP))
            corrected_two = two * (1.0 / (1.0 - beta_two**INNER_STEP))
            held = step[at]
            step[at] = held - inner_rate * (
                corrected_one / (jnp.sqrt(corrected_two) + epsilon) + weight_decay * held
            )

    forward_o(0)
    for load in loads:
        load.wait()
    gathered_o(0)

    last = 0
    for g, c in enumerate(counts):
        for q in range(c):
            j = (g + 1) // 2 if g % 2 else q
            o = chunk_of(j) // halves
            hops = own_lag(o) + max(o, n - 1 - o)
            last = max(last, starts[g] + leads[g] + q + hops * HOP_STEPS + EDGE_LAG)

    def body(t, carry):
        for e in range(1, n):
            pass_on(t, e)
        own(t)
        compute(t)
        wave(t, True)
        wave(t, False)
        return carry

    lax.fori_loop(0, last + 1, body, 0)

    for o in range(n):
        part = from_left.at[:, pl.ds(0, halves)]

        @pl.when(z != o)
        def _():
            pltpu.make_async_copy(part, part, rs_send.at[o]).wait()

        @pl.when((o <= z) & has_right)
        def _():
            pltpu.make_async_copy(part, part, ag_right.at[o]).wait()

        @pl.when((o >= z) & has_left)
        def _():
            pltpu.make_async_copy(part, part, ag_left.at[o]).wait()

    for s in range(ni):
        sent = hbuf.at[s, pl.ds(0, peers - 1)]
        pltpu.make_async_copy(sent, sent, h_send.at[s]).wait()
    for s in range(nj):
        sent = obuf.at[s, pl.ds(0, chips - 1)]
        pltpu.make_async_copy(sent, sent, o_send.at[s]).wait()
        sent = obuf.at[s, pl.ds(0, chips)]
        pltpu.make_async_copy(sent, sent, sib_send.at[s]).wait()


def fused(hidden, out_grad, inner_params, first_moment, second_moment, outer_params, outer_momentum):
    n, peers = lax.axis_size("rep"), lax.axis_size("fsdp")
    tokens = hidden.shape[0]
    rows, width = inner_params.shape
    block = outer_params.shape[1]
    ni, nj = rows // ROW_TILE, width // COL_TILE
    cfg = (n, peers, rows, width, tokens)
    anywhere = pl.BlockSpec(memory_space=pl.ANY)
    vmem = pl.BlockSpec(memory_space=pltpu.VMEM)
    dma = pltpu.SemaphoreType.DMA
    bf16, f32 = jnp.bfloat16, jnp.float32
    return pl.pallas_call(
        functools.partial(fused_kernel, cfg),
        out_shape=(
            pltpu.VMEM((rows, width), f32),
            pltpu.VMEM((rows, block), f32),
            pltpu.VMEM((rows, width), bf16),
            pltpu.VMEM((rows, width), bf16),
        ),
        in_specs=[anywhere] * 7,
        out_specs=(vmem,) * 4,
        scratch_shapes=[
            pltpu.VMEM((ni, peers, tokens, ROW_TILE), bf16),
            pltpu.VMEM((ni, ROW_TILE, peers * tokens), bf16),
            pltpu.VMEM((nj, peers, tokens, COL_TILE), bf16),
            pltpu.VMEM((rows, width), f32),
            pltpu.VMEM((rows, block), f32),
            pltpu.VMEM((rows, width), WIRE),
            pltpu.VMEM((ni, nj, ROW_TILE, COL_TILE), WIRE),
            pltpu.VMEM((ni, nj, ROW_TILE, COL_TILE), WIRE),
            dma((ni,)), dma((ni,)),
            dma((nj,)), dma((nj, peers // 2)), dma((nj,)), dma((nj,)), dma((5,)),
            dma((ni, nj)), dma((ni, nj)), dma((ni, nj)),
            dma((n,)), dma((n,)), dma((n,)),
        ],
        compiler_params=pltpu.CompilerParams(
            collective_id=1, has_side_effects=True, vmem_limit_bytes=VMEM_BYTES
        ),
    )(hidden, out_grad, inner_params, first_moment, second_moment, outer_params, outer_momentum)


def fits(peers, n, rows, width, block, tokens):
    if peers % 4 or rows % ROW_TILE or block % COL_TILE or tokens % 16:
        return False
    return 0 <= width // COL_TILE - rows // ROW_TILE <= 1


def per_device(
    hidden, out_grad, inner_params, first_moment, second_moment, outer_params, outer_momentum
):
    rows, width = inner_params.shape[1:]
    block, tokens = outer_params.shape[1], hidden.shape[0]
    if fits(lax.axis_size("fsdp"), lax.axis_size("rep"), rows, width, block, tokens):
        gathered, new_momentum, new_first, new_second = fused(
            hidden, out_grad, inner_params[0], first_moment[0], second_moment[0],
            outer_params, outer_momentum,
        )
        return gathered, new_momentum, new_first[None], new_second[None]
    columns = lax.all_to_all(hidden, "fsdp", split_axis=1, concat_axis=0, tiled=True)
    segment = lax.all_gather(out_grad, "fsdp", axis=0, tiled=True)
    token_count = hidden.shape[0]
    blocks = segment.shape[0] // token_count
    gradient = jnp.einsum(
        "btf,btd->fd",
        columns.reshape(blocks, token_count, columns.shape[1]),
        segment.reshape(blocks, token_count, segment.shape[1]),
        preferred_element_type=jnp.float32,
    )
    stacked = gradient[None]
    moment_one = beta_one * first_moment.astype(jnp.float32) + (1.0 - beta_one) * stacked
    moment_two = beta_two * second_moment.astype(jnp.float32) + (1.0 - beta_two) * stacked * stacked
    corrected_one = moment_one / (1.0 - beta_one**INNER_STEP)
    corrected_two = moment_two / (1.0 - beta_two**INNER_STEP)
    stepped = inner_params - inner_rate * (
        corrected_one / (jnp.sqrt(corrected_two) + epsilon) + weight_decay * inner_params
    )
    gathered, new_momentum = outer_step(stepped[0], outer_params, outer_momentum)
    return (
        gathered.astype(jnp.float32),
        new_momentum,
        moment_one.astype(jnp.bfloat16),
        moment_two.astype(jnp.bfloat16),
    )


def solution(mesh):
    return jax.shard_map(
        per_device,
        mesh=mesh,
        in_specs=(
            P(("rep", "fsdp"), None),
            P(("rep", "fsdp"), None),
            P("rep", "fsdp", None),
            P("rep", "fsdp", None),
            P("rep", "fsdp", None),
            P("fsdp", "rep"),
            P("fsdp", "rep"),
        ),
        out_specs=(
            P("fsdp", None),
            P("fsdp", "rep"),
            P("rep", "fsdp", None),
            P("rep", "fsdp", None),
        ),
        check_vma=False,
    )
```

```python
import functools

import jax
import jax.numpy as jnp
from jax import lax
from jax.experimental import pallas as pl
from jax.experimental.pallas import tpu as pltpu
from jax.sharding import PartitionSpec as P

INNER_STEP = 500

beta_one = 0.9
beta_two = 0.95
epsilon = 1e-08
inner_rate = 0.0004
weight_decay = 0.1
outer_rate = 0.7
nesterov = 0.9

WIRE = jnp.bfloat16
WIRE_SCALE = 16.0


def encode(value):
    scaled = value * WIRE_SCALE
    square = scaled * scaled
    fourth = square * square
    eighth = fourth * fourth
    return jnp.where(scaled < 0.0, -eighth, eighth).astype(WIRE)


def decode(coded):
    wide = coded.astype(jnp.float32)
    root = jnp.sqrt(jnp.sqrt(jnp.sqrt(jnp.abs(wide)))) * (1.0 / WIRE_SCALE)
    return jnp.where(wide < 0.0, -root, root)


def outer_kernel(
    n, chunks, step_ref, outer_ref, mom_ref, out_ref, newmom_ref,
    from_left, from_right, acc, total,
    rs_send, rs_left, rs_right, ag_right, ag_left, ag_recv,
):
    z = lax.axis_index("rep")
    rows, block = outer_ref.shape
    rc = rows // chunks
    has_left, has_right = z > 0, z < n - 1

    barrier = pltpu.get_barrier_semaphore()

    @pl.when(has_left)
    def _():
        pl.semaphore_signal(barrier, inc=1, device_id={"rep": z - 1})

    @pl.when(has_right)
    def _():
        pl.semaphore_signal(barrier, inc=1, device_id={"rep": z + 1})

    pl.semaphore_wait(barrier, has_left.astype(jnp.int32) + has_right.astype(jnp.int32))

    def part(c, o):
        start = o * block
        if not isinstance(o, int):
            start = pl.multiple_of(start, 128)
        return pl.ds(pl.multiple_of(c * rc, rc), rc), pl.ds(start, block)

    def send_sum(src, c, o, to_right):
        at = part(c, o)
        return pltpu.make_async_remote_copy(
            src_ref=src.at[at],
            dst_ref=(from_left if to_right else from_right).at[at],
            send_sem=rs_send.at[c, o],
            recv_sem=(rs_left if to_right else rs_right).at[c, o],
            device_id={"rep": z + 1 if to_right else z - 1},
        )

    def send_new(c, o, to_right):
        at = part(c, o)
        return pltpu.make_async_remote_copy(
            src_ref=out_ref.at[at],
            dst_ref=out_ref.at[at],
            send_sem=(ag_right if to_right else ag_left).at[c, o],
            recv_sem=ag_recv.at[c, o],
            device_id={"rep": z + 1 if to_right else z - 1},
        )

    def wave(c, to_right):
        first = z == 0 if to_right else z == n - 1
        order = range(n - 1, 0, -1) if to_right else range(n - 1)
        for o in order:
            beyond = o > z if to_right else o < z
            at = part(c, o)

            @pl.when(jnp.logical_and(beyond, first))
            def _():
                acc[at] = encode(step_ref[at])
                send_sum(acc, c, o, to_right).start()

            @pl.when(jnp.logical_and(beyond, jnp.logical_not(first)))
            def _():
                send_sum(acc, c, o, to_right).wait_recv()
                came = (from_left if to_right else from_right)[at]
                acc[at] = encode(decode(came) + step_ref[at])
                send_sum(acc, c, o, to_right).start()

    def own(c):
        at = part(c, z)
        here = pl.ds(pl.multiple_of(c * rc, rc), rc)
        total[...] = step_ref[at]

        @pl.when(has_left)
        def _():
            send_sum(acc, c, z, True).wait_recv()
            total[...] += decode(from_left[at])

        @pl.when(has_right)
        def _():
            send_sum(acc, c, z, False).wait_recv()
            total[...] += decode(from_right[at])

        delta = outer_ref[here, :] - total[...] / n
        momentum = nesterov * mom_ref[here, :] + delta
        newmom_ref[here, :] = momentum
        updated = outer_ref[here, :] - outer_rate * (delta + nesterov * momentum)
        out_ref[at] = updated.astype(WIRE)

        @pl.when(has_right)
        def _():
            send_new(c, z, True).start()

        @pl.when(has_left)
        def _():
            send_new(c, z, False).start()

    def within(c, work):
        @pl.when(jnp.logical_and(c >= 0, c < chunks))
        def _():
            work(c)

    def own_lag(o):
        return jnp.maximum(o, n - 1 - o)

    def forward(t, distance, to_right):
        o = z - distance if to_right else z + distance
        there = o >= 0 if to_right else o < n
        c = t - own_lag(o) - distance
        ready = jnp.logical_and(there, jnp.logical_and(c >= 0, c < chunks))

        @pl.when(ready)
        def _():
            send_new(c, o, to_right).wait_recv()

        @pl.when(jnp.logical_and(ready, has_right if to_right else has_left))
        def _():
            send_new(c, o, to_right).start()

    def body(t, carry):
        within(t - z, lambda c: wave(c, True))
        within(t - (n - 1 - z), lambda c: wave(c, False))
        within(t - own_lag(z), own)
        for distance in range(1, n):
            forward(t, distance, True)
            forward(t, distance, False)
        return carry

    lax.fori_loop(0, chunks + 2 * (n - 1), body, 0)

    def drain(c, carry):
        for o in range(n):
            @pl.when(o > z)
            def _():
                send_sum(acc, c, o, True).wait_send()

            @pl.when(o < z)
            def _():
                send_sum(acc, c, o, False).wait_send()

            @pl.when(jnp.logical_and(o <= z, has_right))
            def _():
                send_new(c, o, True).wait_send()

            @pl.when(jnp.logical_and(o >= z, has_left))
            def _():
                send_new(c, o, False).wait_send()

        return carry

    lax.fori_loop(0, chunks, drain, 0)


def outer_step(stepped, outer_params, outer_momentum):
    n = lax.axis_size("rep")
    rows, block = outer_params.shape
    chunks = max(c for c in range(1, 15) if rows % (16 * c) == 0)
    vmem = pl.BlockSpec(memory_space=pltpu.VMEM)
    dma = pltpu.SemaphoreType.DMA((chunks, n))
    return pl.pallas_call(
        functools.partial(outer_kernel, n, chunks),
        out_shape=(
            jax.ShapeDtypeStruct(stepped.shape, WIRE),
            jax.ShapeDtypeStruct(outer_params.shape, jnp.float32),
        ),
        in_specs=[vmem] * 3,
        out_specs=(vmem, vmem),
        scratch_shapes=[
            pltpu.VMEM(stepped.shape, WIRE),
            pltpu.VMEM(stepped.shape, WIRE),
            pltpu.VMEM(stepped.shape, WIRE),
            pltpu.VMEM((rows // chunks, block), jnp.float32),
            dma, dma, dma, dma, dma, dma,
        ],
        compiler_params=pltpu.CompilerParams(
            collective_id=0, has_side_effects=True, vmem_limit_bytes=40 * 2**20
        ),
    )(stepped, outer_params, outer_momentum)


ROW_TILE = 128
VMEM_BYTES = 40000000
WRITE_BYTES = 20000000
COL_TILE = 256
PIECE = COL_TILE // 2
HOP_STEPS = 4
AHEAD = 2
SEGMENT_STEPS = 6
LEAD = 1
EDGE_LAG = 3
CODE_RANGE = 560.0


def mod(x, k):
    return x & (k - 1) if k & (k - 1) == 0 else x % k


def div(x, k):
    return x >> (k.bit_length() - 1) if k & (k - 1) == 0 else x // k


def fused_kernel(
    cfg,
    hid, og, par_hbm, first_hbm, second_hbm, outer_hbm, mom_hbm,
    wide_ref, mom, first, second,
    hbuf, ht, obuf, step, outer, fresh, from_left, from_right,
    h_send, h_recv, o_send, o_recv, sib_send, sib_recv, load_sem,
    left_sem, right_sem, gather_sem, rs_send, ag_right, ag_left,
):
    n, peers, rows, width, tokens = cfg
    ni, nj = rows // ROW_TILE, width // COL_TILE
    stages = max(ni, nj)
    pairs = n // 2
    halves = nj // n
    chips = peers // 2
    z = lax.axis_index("rep")
    me = lax.axis_index("fsdp")
    core, chip = me % 2, me // 2
    has_left, has_right = z > 0, z < n - 1

    def flag(condition):
        return condition.astype(jnp.int32)

    def peer_chip(d):
        return ((chip // 2 + d // 2) % (chips // 2)) * 2 + (chip + d) % 2

    sibling = chip * 2 + 1 - core

    barrier = pltpu.get_barrier_semaphore()
    for d in range(1, peers):
        target = peer_chip(d // 2) * 2 + (core + d) % 2
        pl.semaphore_signal(barrier, inc=1, device_id={"fsdp": target})

    @pl.when(has_left)
    def _():
        pl.semaphore_signal(barrier, inc=1, device_id={"rep": z - 1})

    @pl.when(has_right)
    def _():
        pl.semaphore_signal(barrier, inc=1, device_id={"rep": z + 1})

    pl.semaphore_wait(barrier, peers - 1 + flag(has_left) + flag(has_right))

    segments = ni + nj - 1
    counts = [(g + 2) // 2 for g in range(segments)]
    leads = [LEAD * (g % 2) for g in range(segments)]
    widths = [
        max(c + a, SEGMENT_STEPS) if g < segments - 1 else c + a
        for g, (c, a) in enumerate(zip(counts, leads))
    ]
    starts = [sum(widths[:g]) for g in range(segments + 1)]
    total_steps = starts[-1]
    even = 0
    while even < segments - 1 and widths[even] == SEGMENT_STEPS:
        even += 1
    inverse = -(-65536 // SEGMENT_STEPS)
    assert all(
        min((u * inverse) >> 16, even) == min(u // SEGMENT_STEPS, even)
        for u in range(total_steps)
    )

    def owner_of(j, h):
        p = mod(j, pairs)
        return pairs + p if h else pairs - 1 - p

    def own_lag(o):
        return max(o, n - 1 - o) if isinstance(o, int) else jnp.maximum(o, n - 1 - o)

    def place(u):
        g = jnp.minimum((u * inverse) >> 16, even)
        base = g * SEGMENT_STEPS
        for a, b in zip(starts[even:-2], starts[even + 1:-1]):
            past = flag(u >= b)
            g = g + past
            base = base + past * (b - a)
        return g, u - base

    def tile(u):
        g, q = place(u)
        odd = g & 1
        half = (g + 1) >> 1
        q = q - LEAD * odd
        i = jnp.where(odd == 1, q, half)
        j = jnp.where(odd == 1, half, q)
        valid = (u >= 0) & (u < total_steps) & (q >= 0) & (q < half + 1 - odd)
        return valid, i, j

    def rows_of(i):
        return pl.ds(pl.multiple_of(i * ROW_TILE, ROW_TILE), ROW_TILE)

    def piece_of(j):
        return pl.ds(pl.multiple_of(div(j, pairs) * PIECE, PIECE), PIECE)

    def cols_of(j, o):
        start = o * (halves * COL_TILE) + div(j, pairs) * PIECE
        return pl.ds(pl.multiple_of(start, PIECE), PIECE)

    def hid_cols(owner, s):
        return pl.ds(pl.multiple_of(owner * rows + s * ROW_TILE, ROW_TILE), ROW_TILE)

    def issue_o(s):
        for h in range(2):
            source = og.at[:, cols_of(s, owner_of(s, h))]
            target = obuf.at[s, me, :, pl.ds(h * PIECE, PIECE)]
            for d in range(1, chips):
                pltpu.make_async_remote_copy(
                    src_ref=source,
                    dst_ref=target,
                    send_sem=o_send.at[s],
                    recv_sem=o_recv.at[s, chip],
                    device_id={"fsdp": peer_chip(d) * 2 + core},
                ).start()
            pltpu.make_async_remote_copy(
                src_ref=source,
                dst_ref=target,
                send_sem=sib_send.at[s],
                recv_sem=sib_recv.at[s],
                device_id={"fsdp": sibling},
            ).start()
            pltpu.make_async_copy(source, target, o_recv.at[s, chip]).start()

    def forward_o(s):
        for d in range(chips):
            source = peer_chip(d)
            block = source * 2 + core
            pltpu.make_async_copy(
                obuf.at[s, block], obuf.at[s, block], o_recv.at[s, source]
            ).wait()
            if d > 0:
                pltpu.make_async_remote_copy(
                    src_ref=obuf.at[s, block],
                    dst_ref=obuf.at[s, block],
                    send_sem=sib_send.at[s],
                    recv_sem=sib_recv.at[s],
                    device_id={"fsdp": sibling},
                ).start()

    def gathered_o(s):
        four = obuf.at[s, pl.ds(0, chips)]
        pltpu.make_async_copy(four, four, sib_recv.at[s]).wait()

    def issue_h(s):
        for d in list(range(2, peers)) + [1]:
            target = peer_chip(d // 2) * 2 + (core + d) % 2
            pltpu.make_async_remote_copy(
                src_ref=hid.at[:, hid_cols(target, s)],
                dst_ref=hbuf.at[s, me],
                send_sem=h_send.at[s],
                recv_sem=h_recv.at[s],
                device_id={"fsdp": target},
            ).start()
        pltpu.make_async_copy(
            hid.at[:, hid_cols(me, s)], hbuf.at[s, me], h_recv.at[s]
        ).start()

    def issue(s):
        if isinstance(s, int):
            if s < nj:
                issue_o(s)
            if s < ni:
                issue_h(s)
        else:
            @pl.when(s < nj)
            def _():
                issue_o(s)

            @pl.when(s < ni)
            def _():
                issue_h(s)

    for s in range(AHEAD):
        issue(s)
    loads = [
        pltpu.make_async_copy(a, b, load_sem.at[k])
        for k, (a, b) in enumerate(
            ((par_hbm, step), (first_hbm, first), (second_hbm, second), (outer_hbm, outer), (mom_hbm, mom))
        )
    ]
    for load in loads:
        load.start()

    def code_scale(terms):
        return CODE_RANGE / terms.astype(jnp.float32)

    def encode(value, terms):
        return jnp.exp(value * code_scale(terms)).astype(WIRE)

    def decode(coded, terms):
        return jnp.log(coded.astype(jnp.float32)) * (1.0 / code_scale(terms))

    def send_sum(i, j, h, o, to_right):
        return pltpu.make_async_remote_copy(
            src_ref=(from_left if to_right else from_right).at[i, j, h],
            dst_ref=(from_left if to_right else from_right).at[i, j, h],
            send_sem=rs_send.at[o],
            recv_sem=(left_sem if to_right else right_sem).at[i, j, h],
            device_id={"rep": z + 1 if to_right else z - 1},
        )

    def send_new(i, j, h, o, to_right):
        return pltpu.make_async_remote_copy(
            src_ref=fresh.at[i, j, h],
            dst_ref=fresh.at[i, j, h],
            send_sem=(ag_right if to_right else ag_left).at[o],
            recv_sem=gather_sem.at[i, j, h],
            device_id={"rep": z + 1 if to_right else z - 1},
        )

    def wave(t, to_right):
        hop = z if to_right else n - 1 - z
        valid, i, j = tile(t - hop * HOP_STEPS)
        partial = from_left if to_right else from_right

        def piece(h):
            o = owner_of(j, h)
            active = valid & ((o > z) if to_right else (o < z))
            at = rows_of(i), cols_of(j, o)

            @pl.when(active & (hop == 0))
            def _():
                partial[i, j, h] = encode(step[at], hop + 1)
                send_sum(i, j, h, o, to_right).start()

            @pl.when(active & (hop > 0))
            def _():
                send_sum(i, j, h, o, to_right).wait_recv()
                partial[i, j, h] = encode(decode(partial[i, j, h], hop) + step[at], hop + 1)
                send_sum(i, j, h, o, to_right).start()

        for h in (1, 0) if to_right else (0, 1):
            piece(h)

    def holds(j, o):
        far = flag(o >= pairs)
        match = jnp.where(far == 1, o - pairs, pairs - 1 - o) == mod(j, pairs)
        return match, far

    def own(t):
        valid, i, j = tile(t - own_lag(z) * HOP_STEPS)
        match, h = holds(j, z)

        @pl.when(valid & match)
        def _():
            at = rows_of(i), cols_of(j, z)
            local = rows_of(i), piece_of(j)

            @pl.when(has_left)
            def _():
                send_sum(i, j, h, z, True).wait_recv()
                step[at] += decode(from_left[i, j, h], z)

            @pl.when(has_right)
            def _():
                send_sum(i, j, h, z, False).wait_recv()
                step[at] += decode(from_right[i, j, h], n - 1 - z)

            delta = outer[local] - step[at] * (1.0 / n)
            momentum = nesterov * mom[local] + delta
            mom[local] = momentum
            updated = outer[local] - outer_rate * (delta + nesterov * momentum)
            fresh[i, j, h] = updated.astype(WIRE)
            wide_ref[at] = updated

            @pl.when(has_right)
            def _():
                send_new(i, j, h, z, True).start()

            @pl.when(has_left)
            def _():
                send_new(i, j, h, z, False).start()

    def pass_on(t, e):
        o = (z + e) % n
        to_right = o < z
        distance = jnp.where(to_right, z - o, o - z)
        edge = jnp.where(to_right, flag(has_right), flag(has_left)) == 0
        lag = (own_lag(o) + distance) * HOP_STEPS + EDGE_LAG * flag(edge)
        valid, i, j = tile(t - lag)
        match, h = holds(j, o)
        at = rows_of(i), cols_of(j, o)

        @pl.when(valid & match)
        def _():
            send_new(i, j, h, o, True).wait_recv()

            @pl.when(to_right & has_right)
            def _():
                send_new(i, j, h, o, True).start()

            @pl.when((o > z) & has_left)
            def _():
                send_new(i, j, h, o, False).start()

            wide_ref[at] = fresh[i, j, h].astype(jnp.float32)

    def compute(t):
        g, q = place(t)
        s = (g + 1) >> 1
        inside = t < total_steps
        valid, i, j = tile(t)

        @pl.when(inside & ((g & 1) == 0) & (q == 0))
        def _():
            issue(s + AHEAD)
            pltpu.make_async_copy(hbuf.at[s], hbuf.at[s], h_recv.at[s]).wait()
            ht[s] = hbuf[s].reshape(peers * tokens, ROW_TILE).T

        @pl.when(inside & ((g & 1) == 1) & (q == 0))
        def _():
            forward_o(s)

        @pl.when(inside & ((g & 1) == 1) & (q == LEAD))
        def _():
            gathered_o(s)

        @pl.when(valid)
        def _():
            gradients = jnp.dot(
                ht[i],
                obuf[j].reshape(peers * tokens, COL_TILE),
                preferred_element_type=jnp.float32,
            )
            for h in range(2):
                at = rows_of(i), cols_of(j, owner_of(j, h))
                gradient = gradients[:, h * PIECE:(h + 1) * PIECE]
                one = beta_one * first[at].astype(jnp.float32) + (1.0 - beta_one) * gradient
                two = (
                    beta_two * second[at].astype(jnp.float32)
                    + (1.0 - beta_two) * gradient * gradient
                )
                first[at] = one.astype(jnp.bfloat16)
                second[at] = two.astype(jnp.bfloat16)
                corrected_one = one * (1.0 / (1.0 - beta_one**INNER_STEP))
                corrected_two = two * (1.0 / (1.0 - beta_two**INNER_STEP))
                held = step[at]
                step[at] = held - inner_rate * (
                    corrected_one / (jnp.sqrt(corrected_two) + epsilon) + weight_decay * held
                )

    forward_o(0)
    for load in loads:
        load.wait()
    gathered_o(0)

    last = 0
    for g, c in enumerate(counts):
        for q in range(c):
            o = owner_of((g + 1) // 2 if g % 2 else q, 0)
            hops = own_lag(o) + max(o, n - 1 - o)
            last = max(last, starts[g] + leads[g] + q + hops * HOP_STEPS + EDGE_LAG)

    def body(t, carry):
        for e in range(1, n):
            pass_on(t, e)
        own(t)
        compute(t)
        wave(t, True)
        wave(t, False)
        return carry

    lax.fori_loop(0, last + 1, body, 0)

    for o in range(n):
        part = from_left.at[:, pl.ds(0, halves)]

        @pl.when(z != o)
        def _():
            pltpu.make_async_copy(part, part, rs_send.at[o]).wait()

        @pl.when((o <= z) & has_right)
        def _():
            pltpu.make_async_copy(part, part, ag_right.at[o]).wait()

        @pl.when((o >= z) & has_left)
        def _():
            pltpu.make_async_copy(part, part, ag_left.at[o]).wait()

    for s in range(ni):
        sent = hbuf.at[s, pl.ds(0, peers - 1)]
        pltpu.make_async_copy(sent, sent, h_send.at[s]).wait()
    for s in range(nj):
        sent = obuf.at[s, pl.ds(0, chips - 1)]
        pltpu.make_async_copy(sent, sent, o_send.at[s]).wait()
        sent = obuf.at[s, pl.ds(0, chips)]
        pltpu.make_async_copy(sent, sent, sib_send.at[s]).wait()


def fused(hidden, out_grad, inner_params, first_moment, second_moment, outer_params, outer_momentum):
    n, peers = lax.axis_size("rep"), lax.axis_size("fsdp")
    tokens = hidden.shape[0]
    rows, width = inner_params.shape
    block = outer_params.shape[1]
    ni, nj = rows // ROW_TILE, width // COL_TILE
    cfg = (n, peers, rows, width, tokens)
    anywhere = pl.BlockSpec(memory_space=pl.ANY)
    vmem = pl.BlockSpec(memory_space=pltpu.VMEM)
    dma = pltpu.SemaphoreType.DMA
    bf16, f32 = jnp.bfloat16, jnp.float32
    return pl.pallas_call(
        functools.partial(fused_kernel, cfg),
        out_shape=(
            pltpu.VMEM((rows, width), f32),
            pltpu.VMEM((rows, block), f32),
            pltpu.VMEM((rows, width), bf16),
            pltpu.VMEM((rows, width), bf16),
        ),
        in_specs=[anywhere] * 7,
        out_specs=(vmem,) * 4,
        scratch_shapes=[
            pltpu.VMEM((ni, peers, tokens, ROW_TILE), bf16),
            pltpu.VMEM((ni, ROW_TILE, peers * tokens), bf16),
            pltpu.VMEM((nj, peers, tokens, COL_TILE), bf16),
            pltpu.VMEM((rows, width), f32),
            pltpu.VMEM((rows, block), f32),
            pltpu.VMEM((ni, nj, 2, ROW_TILE, PIECE), WIRE),
            pltpu.VMEM((ni, nj, 2, ROW_TILE, PIECE), WIRE),
            pltpu.VMEM((ni, nj, 2, ROW_TILE, PIECE), WIRE),
            dma((ni,)), dma((ni,)),
            dma((nj,)), dma((nj, peers // 2)), dma((nj,)), dma((nj,)), dma((5,)),
            dma((ni, nj, 2)), dma((ni, nj, 2)), dma((ni, nj, 2)),
            dma((n,)), dma((n,)), dma((n,)),
        ],
        compiler_params=pltpu.CompilerParams(
            collective_id=1, has_side_effects=True, vmem_limit_bytes=VMEM_BYTES
        ),
    )(hidden, out_grad, inner_params, first_moment, second_moment, outer_params, outer_momentum)


def write_out_kernel(*refs):
    count = (len(refs) - 1) // 2
    sems = refs[-1]
    copies = [
        pltpu.make_async_copy(refs[k], refs[count + k], sems.at[k]) for k in range(count)
    ]
    for copy in copies:
        copy.start()
    for copy in copies:
        copy.wait()


def write_out(*arrays):
    return pl.pallas_call(
        write_out_kernel,
        out_shape=tuple(jax.ShapeDtypeStruct(a.shape, a.dtype) for a in arrays),
        in_specs=[pl.BlockSpec(memory_space=pltpu.VMEM)] * len(arrays),
        out_specs=(pl.BlockSpec(memory_space=pl.ANY),) * len(arrays),
        scratch_shapes=[pltpu.SemaphoreType.DMA((len(arrays),))],
        compiler_params=pltpu.CompilerParams(vmem_limit_bytes=WRITE_BYTES),
    )(*arrays)


def fits(peers, n, rows, width, block, tokens):
    if peers % 4 or n % 2 or rows % ROW_TILE or block % COL_TILE or tokens % 16:
        return False
    return 0 <= width // COL_TILE - rows // ROW_TILE <= 1


def per_device(
    hidden, out_grad, inner_params, first_moment, second_moment, outer_params, outer_momentum
):
    rows, width = inner_params.shape[1:]
    block, tokens = outer_params.shape[1], hidden.shape[0]
    if fits(lax.axis_size("fsdp"), lax.axis_size("rep"), rows, width, block, tokens):
        gathered, new_momentum, new_first, new_second = fused(
            hidden, out_grad, inner_params[0], first_moment[0], second_moment[0],
            outer_params, outer_momentum,
        )
        gathered, new_momentum, new_first, new_second = write_out(
            gathered, new_momentum, new_first, new_second
        )
        return gathered, new_momentum, new_first[None], new_second[None]
    columns = lax.all_to_all(hidden, "fsdp", split_axis=1, concat_axis=0, tiled=True)
    segment = lax.all_gather(out_grad, "fsdp", axis=0, tiled=True)
    token_count = hidden.shape[0]
    blocks = segment.shape[0] // token_count
    gradient = jnp.einsum(
        "btf,btd->fd",
        columns.reshape(blocks, token_count, columns.shape[1]),
        segment.reshape(blocks, token_count, segment.shape[1]),
        preferred_element_type=jnp.float32,
    )
    stacked = gradient[None]
    moment_one = beta_one * first_moment.astype(jnp.float32) + (1.0 - beta_one) * stacked
    moment_two = beta_two * second_moment.astype(jnp.float32) + (1.0 - beta_two) * stacked * stacked
    corrected_one = moment_one / (1.0 - beta_one**INNER_STEP)
    corrected_two = moment_two / (1.0 - beta_two**INNER_STEP)
    stepped = inner_params - inner_rate * (
        corrected_one / (jnp.sqrt(corrected_two) + epsilon) + weight_decay * inner_params
    )
    gathered, new_momentum = outer_step(stepped[0], outer_params, outer_momentum)
    return (
        gathered.astype(jnp.float32),
        new_momentum,
        moment_one.astype(jnp.bfloat16),
        moment_two.astype(jnp.bfloat16),
    )


def solution(mesh):
    return jax.shard_map(
        per_device,
        mesh=mesh,
        in_specs=(
            P(("rep", "fsdp"), None),
            P(("rep", "fsdp"), None),
            P("rep", "fsdp", None),
            P("rep", "fsdp", None),
            P("rep", "fsdp", None),
            P("fsdp", "rep"),
            P("fsdp", "rep"),
        ),
        out_specs=(
            P("fsdp", None),
            P("fsdp", "rep"),
            P("rep", "fsdp", None),
            P("rep", "fsdp", None),
        ),
        check_vma=False,
    )
```
